32 devices in a mesh: run: 2 (over y), gx: 4 (over x, core), gy: 4 (over z).
Axes of the slice: x: 2, y: 2, z: 4, core: 2. Of those that a mesh axis runs over, the one named last changes fastest.
Arguments:
- magnet: float32 [3, 4, 256, 256], P(None, None, ('run', 'gx', 'gy')), parts along dimension 2, may hold values from -1 to 1, as said below
- window_shift: int32 [2], P('run'), parts along dimension 0, may hold values from 1 to 7
- region: int32 [256, 256], P(('run', 'gx', 'gy')), parts along dimension 0, may hold values 0 or 1
- material: float32 [4, 5], replicated, may hold values from 0.1 to 1
- kernel: float32 [6, 7, 256, 256], P(None, None, ('gx', 'gy')), may hold values from -6 to 6, as said below
Outputs:
- magnet_next: float32 [3, 4, 256, 256], P(None, None, ('run', 'gx', 'gy')), parts along dimension 2
- effective_field: float32 [3, 4, 256, 256], P(None, None, ('run', 'gx', 'gy')), parts along dimension 2
The draws below stay inside these ranges and needn't reach their ends.
There are 2 independent parts, one for each index of `run`. The reference program is written for one: setup_inputs(seed, part) draws one part's arguments, and reference() takes and returns one part's arrays. A program takes and returns all parts, laid end to end along the dimension named above; an argument that names none is the same for every part. Nothing has to cross between parts.
Inputs may be any that keep to these rules, and one draw needn't show every extreme that they name: `magnet`: each cell's three components form a unit vector. kernel[c, d, ky, kx] equals t_c kernel[c, d, ky, (256 - kx) mod 256] with t_c = -1 for c = 3 and 4, 1 otherwise; it equals u_c kernel[c, 6 - d, ky, kx] with u_c = -1 for c = 4 and 5, 1 otherwise; components 3 and 5 are zero at ky = 0.
All inputs are finite; a program needn't handle non-finite values. No bound on the sum of `region` on one device may be relied on, other than what follows from the above.
Results may differ from the reference program's by a relative error of at most 0.0001.
Values sent between devices are 32-bit elements; how exact they have to be, the bound alone decides.
A program may use at most 128 MiB of HBM per device.

```python
import math
import jax
import jax.numpy as jnp
import numpy as np
from jax import lax

CX = 8
NY = 256
NZ = 4
NX = 128
KX = 256
KY = 511
DZ = 7


def draw_magnet(key, part):
    key_height, key_angle = jax.random.split(key)
    shape = (NZ, NX, NY)
    height = jax.random.uniform(key_height, shape, jnp.float32, -0.98, 0.98)
    angles = jax.random.uniform(key_angle, shape, jnp.float32, -math.pi, math.pi)
    radial = jnp.sqrt(1.0 - height * height)
    return jnp.stack([radial * jnp.cos(angles), radial * jnp.sin(angles), height]).astype(jnp.float32)


def draw_kernel(key, part):
    shape = (6, DZ, NY, KX)
    sample = jnp.clip(2.0 * jax.random.normal(key, shape, jnp.float32), -6.0, 6.0)
    track_sign = jnp.array([1.0, 1.0, 1.0, -1.0, -1.0, 1.0], jnp.float32).reshape(6, 1, 1, 1)
    layer_sign = jnp.array([1.0, 1.0, 1.0, 1.0, -1.0, -1.0], jnp.float32).reshape(6, 1, 1, 1)
    width_sign = jnp.array([1.0, 1.0, 1.0, -1.0, 1.0, -1.0], jnp.float32).reshape(6, 1, 1, 1)
    flipped = jnp.roll(jnp.flip(sample, 3), 1, 3)
    even_track = 0.5 * (sample + track_sign * flipped)
    parity = 0.5 * (even_track + layer_sign * jnp.flip(even_track, 1))
    kept_rows = (width_sign > 0.0) | (jnp.arange(NY) > 0)[None, None, :, None]
    return jnp.where(kept_rows, parity, 0.0).astype(jnp.float32)


def with_ends(result, rng, smallest, high):
    longest = result.shape.index(max(result.shape))
    spots = []
    for shift in (0, 1):
        where = [jax.random.randint(jax.random.fold_in(rng, axis), (), 0, length) for axis, length in enumerate(result.shape)]
        where[longest] = (where[longest] + shift) % result.shape[longest]
        spots.append(tuple(where))
    return result.at[spots[0]].set(smallest).at[spots[1]].set(high)


def setup_inputs(seed: int = 0, part: int = 0) -> dict:
    streams_of = jax.random.split(jax.random.key(seed), 6)
    own_keys = jax.random.split(jax.random.fold_in(streams_of[5], part), 6)
    return {
        "magnet": draw_magnet(jax.random.fold_in(jax.random.fold_in(streams_of[5], part), 71), part),
        "window_shift": jax.random.randint(own_keys[1], (1,), 1, CX).astype(jnp.int32),
        "region": with_ends((jax.random.randint(own_keys[2], (NX, NY), 0, 4) < 3).astype(jnp.int32), jax.random.fold_in(own_keys[2], 1), 0, 1),
        "material": jnp.clip(jnp.exp(jax.random.uniform(streams_of[3], (NZ, 5), jnp.float32, math.log(0.1), math.log(1.0))), 0.1, 1.0),
        "kernel": draw_kernel(jax.random.fold_in(streams_of[5], 71), part),
    }


time_step = 0.1
pair_comp = ((0, 3, 4), (3, 1, 5), (4, 5, 2))


def cross_product(left, right):
    return jnp.stack([left[1] * right[2] - left[2] * right[1],
                      left[2] * right[0] - left[0] * right[2],
                      left[0] * right[1] - left[1] * right[0]])


def neighbours(state):
    padded = jnp.pad(state, ((0, 0), (1, 1), (1, 1), (1, 1)), mode="edge")
    laplace = padded[:, 2:, 1:-1, 1:-1] + padded[:, :-2, 1:-1, 1:-1]
    laplace = laplace + padded[:, 1:-1, 2:, 1:-1] + padded[:, 1:-1, :-2, 1:-1]
    laplace = laplace + padded[:, 1:-1, 1:-1, 2:] + padded[:, 1:-1, 1:-1, :-2] - 6.0 * state
    slope = 0.5 * (padded[:, 1:-1, 2:, 1:-1] - padded[:, 1:-1, :-2, 1:-1])
    return laplace, slope


def demag_field(state, kernel_full):
    dz_table = np.arange(NZ)[:, None] - np.arange(NZ)[None, :] + NZ - 1
    turned = jnp.transpose(state, (0, 1, 3, 2))
    spectrum = jnp.fft.fft2(turned, s=(KY, KX), axes=(2, 3))
    real_in = jnp.real(spectrum)
    imag_in = jnp.imag(spectrum)
    comps = []
    for i in range(3):
        real_sum = jnp.zeros((NZ, KY, KX), jnp.float32)
        imag_sum = jnp.zeros((NZ, KY, KX), jnp.float32)
        for j in range(3):
            index_c = pair_comp[i][j]
            pairs = kernel_full[index_c][dz_table]
            real_term = jnp.einsum("zwab,wab->zab", pairs, real_in[j], precision=lax.Precision.HIGHEST)
            imag_term = jnp.einsum("zwab,wab->zab", pairs, imag_in[j], precision=lax.Precision.HIGHEST)
            if index_c >= 4:
                real_sum = real_sum - imag_term
                imag_sum = imag_sum + real_term
            else:
                real_sum = real_sum + real_term
                imag_sum = imag_sum + imag_term
        inverse = jnp.fft.ifft2(lax.complex(real_sum, imag_sum), axes=(1, 2))
        comps.append(jnp.real(inverse)[:, :NY, :NX])
    return jnp.transpose(jnp.stack(comps), (0, 1, 3, 2))


def reference(magnet, window_shift, region, material, kernel):
    width_sign = jnp.array([1.0, 1.0, 1.0, -1.0, 1.0, -1.0], jnp.float32).reshape(6, 1, 1, 1)
    mirrored = width_sign * jnp.flip(kernel[:, :, 1:], axis=2)
    kernel_full = jnp.concatenate([kernel, mirrored], axis=2)
    offset = window_shift[0]
    padded = jnp.concatenate([magnet, jnp.zeros((3, NZ, CX, NY), jnp.float32)], axis=2)
    moved = lax.dynamic_slice_in_dim(padded, offset, NX, 2)
    cells = jnp.arange(NX, dtype=jnp.int32)
    fill_up = (jnp.arange(3) == 2).astype(jnp.float32).reshape(3, 1, 1, 1)
    window = jnp.where((cells >= NX - offset)[None, None, :, None], fill_up, moved)
    damping = material[:, 0].reshape(1, NZ, 1, 1)
    nonadiabatic = material[:, 1].reshape(1, NZ, 1, 1)
    stiffness = material[:, 2].reshape(1, NZ, 1, 1)
    anisotropy = material[:, 3].reshape(1, NZ, 1, 1)
    drift_speed = material[:, 4].reshape(1, NZ, 1, 1) * region.astype(jnp.float32)[None, None]

    def rate_of(state):
        laplace, slope = neighbours(state)
        effective = stiffness * laplace + anisotropy * state[2:3] * fill_up + demag_field(state, kernel_full)
        drift_term = drift_speed * slope
        torque_h = cross_product(state, effective)
        damping_h = cross_product(state, torque_h)
        torque_u = cross_product(state, drift_term)
        damping_u = cross_product(state, torque_u)
        change = (-torque_h - damping * damping_h + (1.0 + damping * nonadiabatic) * damping_u
                  + (nonadiabatic - damping) * torque_u) / (1.0 + damping * damping)
        return change, effective

    section_one, effective_field = rate_of(window)
    section_two, _ = rate_of(window + 0.5 * time_step * section_one)
    section_three, _ = rate_of(window + 0.5 * time_step * section_two)
    section_four, _ = rate_of(window + time_step * section_three)
    magnet_next = window + (time_step / 6.0) * (section_one + 2.0 * section_two + 2.0 * section_three + section_four)
    return magnet_next, effective_field
```

```python
import functools
import math

import jax
import jax.numpy as jnp
import numpy as np
from jax import lax
from jax.experimental import pallas as pl
from jax.experimental.pallas import tpu as pltpu
from jax.sharding import PartitionSpec as P

time_step = 0.1
pair_comp = ((0, 3, 4), (3, 1, 5), (4, 5, 2))
lane_tile = 128
f32, bf16 = jnp.float32, jnp.bfloat16


def split_table(table):
    high = table.astype(bf16)
    low = (table - high.astype(np.float64)).astype(bf16)
    return np.stack([high, low])


def width_tables(width, devices, track_freq):
    length = 2 * width - 1
    angle = 2.0 * math.pi / length * (np.arange(width)[:, None] * np.arange(width)[None, :] % length)
    both = np.stack([np.cos(angle), -np.sin(angle)], axis=1)
    both = both.reshape(width, 2, devices, width // devices).transpose(0, 2, 1, 3)
    forward = both.reshape(width, 2 * width)
    weight = np.where(np.arange(width) == 0, 1.0, 2.0).reshape(devices, 1, width // devices)
    inverse = (both * weight).reshape(width, 2 * width).T / (2.0 * track_freq * length)
    return split_table(forward), split_table(inverse)


def track_tables(cells):
    freq = 2 * cells
    angle = 2.0 * math.pi / freq * (np.arange(cells)[:, None] * np.arange(cells)[None, :] % freq)
    cosine, sine = np.cos(angle), np.sin(angle)
    sine[:, 0] = np.where(np.arange(cells) % 2 == 0, 1.0, -1.0)
    forward = np.concatenate([cosine, sine], axis=1)
    weight = np.where(np.arange(freq) % cells == 0, 1.0, 2.0)[:, None]
    return split_table(forward), split_table(forward.T * weight)


def product(values, table):
    rows = values.shape[0]
    high = values.astype(bf16)
    low = (values - high.astype(f32)).astype(bf16)
    first = jnp.dot(jnp.concatenate([high, low], axis=0), table[0], preferred_element_type=f32)
    second = jnp.dot(high, table[1], preferred_element_type=f32)
    return first[:rows] + first[rows:] + second


def turned(power, parts):
    real, imag = parts
    return ((real, imag), (-imag, real), (-real, -imag), (imag, -real))[power % 4]


def kernel_body(
    grid_y, devices, layers,
    *refs,
):
    hbm_refs, shift_cell, (next_ref, field_ref), loaded, load_sems, rest = (
        refs[:8], refs[8], refs[9:11], refs[11:19], refs[19], refs[20:]
    )
    magnet_ref, fwd_y, kernel_ref, inv_y, fwd_t, inv_t, material_ref, region_ref = loaded
    loads = [
        pltpu.make_async_copy(source, target, load_sems.at[n])
        for n, (source, target) in enumerate(zip(hbm_refs, loaded))
    ]
    for load in loads:
        load.start()
    run_step(
        grid_y, devices, layers, loads, shift_cell, material_ref, magnet_ref, region_ref,
        kernel_ref, fwd_y, inv_y, fwd_t, inv_t, next_ref, field_ref, *rest,
    )


def run_step(
    grid_y, devices, layers, loads,
    shift_ref, material_ref, magnet_ref, region_ref, kernel_ref, fwd_y, inv_y, fwd_t, inv_t,
    next_ref, field_ref,
    joined, initial, state, local_field, slope_ref, halo_out, halo_in, spec, table,
    send_a, recv_a, send_b, recv_b, track_hat, track_prod,
    fill_ref, win_sem, halo_sems, a_send_sem, a_recv_sem, b_send_sem, b_recv_sem,
):
    fields, rows, width = state.shape
    half = layers // 2
    freqs = kernel_ref.shape[2]
    track = devices * rows
    block = 2 * freqs
    groups, _, _, padded = send_a.shape
    group_fields = fields // groups
    group_rows = group_fields * block
    me = lax.axis_index("gx") * grid_y + lax.axis_index("gy")

    def device_of(peer):
        return {"gx": peer // grid_y, "gy": lax.rem(peer, grid_y)}

    def peer_at(offset):
        return lax.rem(me + offset, devices)

    right, left = peer_at(1), peer_at(devices - 1)
    grid_x = devices // grid_y
    my_x, my_y = lax.axis_index("gx"), lax.axis_index("gy")
    others = []
    for k in range(grid_y - 1):
        high, low = grid_y - 1 - k, k
        far_y = jnp.where(
            my_y < grid_y // 2,
            high - jnp.where(my_y >= high, 1, 0),
            low + jnp.where(my_y <= low, 1, 0),
        )
        others += [(lax.rem(my_x + a, grid_x), far_y) for a in range(grid_x)]
    others += [(lax.rem(my_x + a, grid_x), my_y) for a in range(1, grid_x)]

    others = others[::-1]
    barrier = pltpu.get_barrier_semaphore()
    for offset in range(1, devices):
        pl.semaphore_signal(barrier, inc=1, device_id=device_of(peer_at(offset)))

    lane_small = lax.broadcasted_iota(jnp.int32, (rows, lane_tile), 1)

    def place(c, sign, z):
        return ((sign ^ (c == 2)) * 3 + c) * half + z

    tiles_all = padded // lane_tile
    cut_a = -(-3 * half * block // lane_tile)
    cut_b = 3 * half * block // lane_tile
    parts_a = [part for part in ((0, cut_a), (cut_a, tiles_all)) if part[0] < part[1]]
    parts_b = [part for part in ((0, cut_b), (cut_b, tiles_all)) if part[0] < part[1]]

    def lanes(part):
        return pl.ds(part[0] * lane_tile, (part[1] - part[0]) * lane_tile)

    def in_block(start):
        return (lane_small >= start) & (lane_small < start + block)

    def halo_copies(step):
        return [
            pltpu.make_async_remote_copy(
                src_ref=halo_out.at[side], dst_ref=halo_in.at[lax.rem(step, 2), 1 - side],
                send_sem=halo_sems.at[lax.rem(step, 2), 0, side],
                recv_sem=halo_sems.at[lax.rem(step, 2), 1, 1 - side],
                device_id=device_of(peer),
            )
            for side, peer in ((0, left), (1, right))
        ]

    def exchange(source, target, send_sem, recv_sem, parts, n, other):
        peer = other[0] * grid_y + other[1]
        return pltpu.make_async_remote_copy(
            src_ref=source.at[0, peer, :, lanes(parts[n])],
            dst_ref=target.at[0, me, :, lanes(parts[n])],
            send_sem=send_sem.at[n], recv_sem=recv_sem.at[n],
            device_id={"gx": other[0], "gy": other[1]},
        )

    def all_blocks(source, target, send_sem, recv_sem, parts, n):
        others = pl.ds(0, devices - 1)
        return pltpu.make_async_remote_copy(
            src_ref=source.at[0, others, :, lanes(parts[n])],
            dst_ref=target.at[0, others, :, lanes(parts[n])],
            send_sem=send_sem.at[n], recv_sem=recv_sem.at[n],
            device_id=device_of(right),
        )

    a_refs = (send_a, recv_a, a_send_sem, a_recv_sem, parts_a)
    b_refs = (send_b, recv_b, b_send_sem, b_recv_sem, parts_b)

    def width_blocks(values, target):
        for group in range(groups):
            spec[...] = product(
                jnp.concatenate(
                    values[group * group_fields : (group + 1) * group_fields], axis=0
                ),
                fwd_y,
            )
            for d in range(devices):
                tile, start = divmod(d * block, lane_tile)
                tiles = [jnp.zeros((rows, lane_tile), f32)] * (padded // lane_tile)
                for f in range(group_fields):
                    to_tile, to_start = divmod(f * block, lane_tile)
                    piece = spec[pl.ds(f * rows, rows), pl.ds(tile * lane_tile, lane_tile)]
                    if to_start != start:
                        piece = pltpu.roll(piece, (to_start - start) % lane_tile, 1)
                    tiles[to_tile] = jnp.where(in_block(to_start), piece, tiles[to_tile])
                for t, value in enumerate(tiles):
                    target[group, d, :, pl.ds(t * lane_tile, lane_tile)] = value

    def mirrored(cells):
        values = [None] * fields
        for c in range(3):
            for z in range(half):
                a, b = cells[c * layers + z], cells[c * layers + layers - 1 - z]
                values[place(c, 0, z)] = a + b
                values[place(c, 1, z)] = a - b
        return values

    def send_forward():
        for n in range(len(parts_a)):
            for o in others:
                exchange(*a_refs, n, o).start()
        recv_a[0, me] = send_a[0, me]

    for load in loads[:2]:
        load.wait()
    width_blocks(mirrored(magnet_ref), send_a)
    pl.semaphore_wait(barrier, devices - 1)
    send_forward()
    window_copy = pltpu.make_async_remote_copy(
        src_ref=magnet_ref, dst_ref=joined.at[:, pl.ds(rows, rows)],
        send_sem=win_sem.at[0], recv_sem=win_sem.at[1], device_id=device_of(left),
    )
    window_copy.start()

    joined[:, pl.ds(0, rows)] = magnet_ref[...]
    fill_values = [
        jnp.full((rows, width), 2.0 if f // half == 5 else 0.0, f32) for f in range(fields)
    ]
    width_blocks(fill_values, send_b)
    fill_ref[...] = send_b[:, me]
    for load in loads[2:]:
        load.wait()
    lane_track = lax.broadcasted_iota(jnp.int32, (freqs, track), 1)
    for c in range(6):
        for z in range(half):
            for w in range(half):
                near = kernel_ref[c, layers - 1 + z - w]
                far = kernel_ref[c, 2 * layers - 2 - z - w]
                for sign, value in enumerate((near + far, near - far)):
                    cosines = value[:, :track]
                    table[c, z, w, sign, :, pl.ds(0, track)] = cosines
                    table[c, z, w, sign, :, pl.ds(track, track)] = jnp.where(
                        lane_track == 0, value[:, track:], cosines
                    )
    if padded > group_rows:
        track_prod[...] = jnp.zeros_like(track_prod)

    offset = shift_ref[0]
    row_index = lax.broadcasted_iota(jnp.int32, (rows, width), 0)
    lane_index = lax.broadcasted_iota(jnp.int32, (rows, width), 1)
    beyond = track - offset

    def set_window():
        window_copy.wait()
        for f in range(fields):
            fill = 1.0 if f // layers == 2 else 0.0
            moved = pltpu.roll(joined[f], 2 * rows - offset, 0)
            cells = jnp.where(me * rows + row_index >= beyond, fill, moved[:rows])
            initial[f] = cells
            state[f] = cells
            next_ref[f] = cells
            halo_in[0, 0, pl.ds(f, 1), :] = jnp.where(
                me * rows - 1 >= beyond, fill, moved[2 * rows - 1 :]
            )
            halo_in[0, 1, pl.ds(f, 1), :] = jnp.where(
                me * rows + rows >= beyond, fill, moved[rows : rows + 1]
            )

    def stage(step, carry):
        def arrive(n):
            all_blocks(*a_refs, n).wait_recv()
            part = lanes(parts_a[n])

            @pl.when(step == 0)
            def _():
                whole = recv_a[0, :, :, part].reshape(track, part.size)
                moved = pltpu.roll(whole, track - offset, 0)
                cell = lax.broadcasted_iota(jnp.int32, moved.shape, 0)
                moved = jnp.where(cell >= beyond, fill_ref[0, pl.ds(0, 1), part], moved)
                recv_a[0, :, :, part] = moved.reshape(devices, rows, part.size)

            arrived = recv_a[0, :, :, part].reshape(track, part.size)
            track_hat[part] = product(arrived.T, fwd_t)

        def give_back(n):
            part = lanes(parts_b[n])
            back = product(track_prod[part], inv_t).T
            send_b[0, :, :, part] = back.reshape(devices, rows, part.size)
            for o in others:
                exchange(*b_refs, n, o).start()
            recv_b[0, me, :, part] = send_b[0, me, :, part]

        def hat(c, sign, z, odd):
            first = place(c, sign, z) * block
            return tuple(
                track_hat[pl.ds(first + p * freqs, freqs), pl.ds(odd * track, track)]
                for p in range(2)
            )

        for chosen in range(2):
            if chosen < len(parts_a):
                arrive(chosen)
            for i in range(3):
                sign = chosen ^ (i == 2)
                for z in range(half):
                    for odd in range(2):
                        total = [None, None]
                        for j in range(3):
                            c = pair_comp[i][j]
                            power = 1 if c >= 4 else 0
                            swap = c in (3, 4)
                            if swap:
                                power += 1 if odd else 3
                            for w in range(half):
                                tab = table[c, z, w, sign, :, pl.ds(odd * track, track)]
                                source = hat(
                                    j, sign ^ (c >= 4), w, 1 - odd if swap else odd
                                )
                                parts = turned(power, tuple(tab * value for value in source))
                                total = [
                                    part if old is None else old + part
                                    for old, part in zip(total, parts)
                                ]
                        first = place(i, sign, z) * block
                        for p in range(2):
                            track_prod[
                                pl.ds(first + p * freqs, freqs), pl.ds(odd * track, track)
                            ] = total[p]

            if chosen == 1 or len(parts_b) == 2:
                give_back(min(chosen, len(parts_b) - 1))

        @pl.when(step == 0)
        def _():
            set_window()

        @pl.when(step > 0)
        def _():
            for copy in halo_copies(step):
                copy.wait()

        turn = lax.rem(step, 2)

        flow = region_ref[...].astype(f32)
        for z in range(layers):
            drift = material_ref[z, 4] * flow
            for c in range(3):
                f = c * layers + z
                cells = state[f]
                before = jnp.where(me == 0, cells[0:1], halo_in[turn, 0, pl.ds(f, 1), :])
                after = jnp.where(
                    me == devices - 1, cells[rows - 1 : rows], halo_in[turn, 1, pl.ds(f, 1), :]
                )
                up = jnp.where(row_index == 0, before, pltpu.roll(cells, 1, 0))
                down = jnp.where(row_index == rows - 1, after, pltpu.roll(cells, rows - 1, 0))
                side_a = jnp.where(lane_index == 0, cells, pltpu.roll(cells, 1, 1))
                side_b = jnp.where(
                    lane_index == width - 1, cells, pltpu.roll(cells, width - 1, 1)
                )
                below = state[c * layers + max(z - 1, 0)]
                above = state[c * layers + min(z + 1, layers - 1)]
                laplace = up + down + side_a + side_b + below + above - 6.0 * cells
                effective = material_ref[z, 2] * laplace
                if c == 2:
                    effective = effective + material_ref[z, 3] * cells
                local_field[f] = effective
                slope_ref[f] = drift * (0.5 * (down - up))

        demag = []
        for group in range(groups):
            for f in range(group_fields):
                from_tile, from_start = divmod(f * block, lane_tile)
                for n, part in enumerate(parts_b):
                    if from_start == 0 and from_tile == part[0]:
                        all_blocks(*b_refs, n).wait_recv()
                tiles = [None] * (2 * width // lane_tile)
                for d in range(devices):
                    tile, start = divmod(d * block, lane_tile)
                    piece = recv_b[group, d, :, pl.ds(from_tile * lane_tile, lane_tile)]
                    if from_start != start:
                        piece = pltpu.roll(piece, (start - from_start) % lane_tile, 1)
                    old = tiles[tile]
                    tiles[tile] = piece if old is None else jnp.where(in_block(start), piece, old)
                for t, value in enumerate(tiles):
                    spec[pl.ds(f * rows, rows), pl.ds(t * lane_tile, lane_tile)] = value
            field = product(spec[...], inv_y)
            demag += [field[f * rows : (f + 1) * rows] for f in range(group_fields)]

        weight = jnp.where((step == 0) | (step == 3), time_step / 6.0, time_step / 3.0)
        ahead = jnp.where(step == 2, time_step, 0.5 * time_step)

        def demag_of(c, sign, z):
            return demag[place(c, sign, z)]

        for z in range(layers):
            mirror = min(z, layers - 1 - z)
            m, h, g = [], [], []
            for c in range(3):
                f = c * layers + z
                even, odd = demag_of(c, 0, mirror), demag_of(c, 1, mirror)
                value = local_field[f] + (even + odd if z < half else even - odd)

                @pl.when(step == 0)
                def _():
                    field_ref[f] = value

                m.append(state[f])
                h.append(value)
                g.append(slope_ref[f])

            def cross(a, b):
                return [
                    a[1] * b[2] - a[2] * b[1],
                    a[2] * b[0] - a[0] * b[2],
                    a[0] * b[1] - a[1] * b[0],
                ]

            damping = jnp.full((rows, width), material_ref[z, 0], f32)
            adiabatic = material_ref[z, 1]
            scale = 1.0 / (1.0 + damping * damping)
            torque_h, torque_u = cross(m, h), cross(m, g)
            inner = [
                (1.0 + damping * adiabatic) * u - damping * t for t, u in zip(torque_h, torque_u)
            ]
            outer = cross(m, inner)
            for c in range(3):
                f = c * layers + z
                change = (outer[c] - torque_h[c] + (adiabatic - damping) * torque_u[c]) * scale
                next_ref[f] = next_ref[f] + weight * change
                state[f] = initial[f] + ahead * change

        for refs in (a_refs, b_refs):
            for n in range(len(refs[-1])):
                all_blocks(*refs, n).wait_send()

        @pl.when(step < 3)
        def _():
            width_blocks(mirrored(state), send_a)
            send_forward()
            for f in range(fields):
                halo_out[0, pl.ds(f, 1), :] = state[f, pl.ds(0, 1), :]
                halo_out[1, pl.ds(f, 1), :] = state[f, pl.ds(rows - 1, 1), :]
            for copy in halo_copies(step + 1):
                copy.start()

        return carry

    lax.fori_loop(0, 4, stage, 0)


def local(magnet, window_shift, region, material, kernel):
    components, layers, rows, width = magnet.shape
    grid_y = lax.axis_size("gy")
    devices = lax.axis_size("gx") * grid_y
    fields = components * layers
    track = rows * devices
    freqs = kernel.shape[2]
    groups = 1
    padded = -(-fields // groups * 2 * freqs // lane_tile) * lane_tile
    tables = (*width_tables(width, devices, 2 * track), *track_tables(track))
    vmem = pl.BlockSpec(memory_space=pltpu.VMEM)
    cells = (fields, rows, width)
    half = layers // 2
    blocks = (groups, devices, rows, padded)
    out = pltpu.VMEM(cells, f32)
    dma = pltpu.SemaphoreType.DMA
    magnet_next, field = pl.pallas_call(
        functools.partial(kernel_body, grid_y, devices, layers),
        out_shape=(out, out),
        in_specs=[pl.BlockSpec(memory_space=pltpu.HBM)] * 8 + [pl.BlockSpec(memory_space=pltpu.SMEM)],
        out_specs=(vmem, vmem),
        scratch_shapes=[
            pltpu.VMEM(cells, f32),
            pltpu.VMEM(tables[0].shape, bf16),
            pltpu.VMEM(kernel.shape, f32),
            *[pltpu.VMEM(table.shape, bf16) for table in tables[1:]],
            pltpu.SMEM(material.shape, f32),
            pltpu.VMEM(region.shape, jnp.int32),
            dma((8,)),
            pltpu.VMEM((fields, 2 * rows, width), f32),
            pltpu.VMEM(cells, f32),
            pltpu.VMEM(cells, f32),
            pltpu.VMEM(cells, f32),
            pltpu.VMEM(cells, f32),
            pltpu.VMEM((2, fields, width), f32),
            pltpu.VMEM((2, 2, fields, width), f32),
            pltpu.VMEM((fields // groups * rows, 2 * width), f32),
            pltpu.VMEM((6, half, half, 2, freqs, 2 * track), f32),
            pltpu.VMEM(blocks, f32),
            pltpu.VMEM(blocks, f32),
            pltpu.VMEM(blocks, f32),
            pltpu.VMEM(blocks, f32),
            pltpu.VMEM((groups * padded, 2 * track), f32),
            pltpu.VMEM((groups * padded, 2 * track), f32),
            pltpu.VMEM((groups, rows, padded), f32),
            dma((2,)),
            dma((2, 2, 2)),
            dma((2,)),
            dma((2,)),
            dma((2,)),
            dma((2,)),
        ],
        compiler_params=pltpu.CompilerParams(
            collective_id=0, has_side_effects=True, vmem_limit_bytes=60 * 2**20
        ),
    )(
        magnet.reshape(cells),
        jnp.asarray(tables[0]),
        kernel,
        *[jnp.asarray(table) for table in tables[1:]],
        material,
        region,
        window_shift,
    )
    return magnet_next.reshape(magnet.shape), field.reshape(magnet.shape)


def solution(mesh):
    cells = P(None, None, ("run", "gx", "gy"), None)
    in_specs = (
        cells,
        P("run"),
        P(("run", "gx", "gy"), None),
        P(),
        P(None, None, ("gx", "gy"), None),
    )
    return jax.shard_map(
        local, mesh=mesh, in_specs=in_specs, out_specs=(cells, cells), check_vma=False
    )
```

```python
import functools
import math

import jax
import jax.numpy as jnp
import numpy as np
from jax import lax
from jax.experimental import pallas as pl
from jax.experimental.pallas import tpu as pltpu
from jax.sharding import PartitionSpec as P

time_step = 0.1
pair_comp = ((0, 3, 4), (3, 1, 5), (4, 5, 2))
lane_tile = 128
f32, bf16 = jnp.float32, jnp.bfloat16


def split_table(table):
    high = table.astype(bf16)
    low = (table - high.astype(np.float64)).astype(bf16)
    return np.concatenate([high, low], axis=1)


def deep(table):
    return np.concatenate([table, table], axis=0)


def width_tables(width, devices, track_freq):
    length = 2 * width - 1
    angle = 2.0 * math.pi / length * (np.arange(width)[:, None] * np.arange(width)[None, :] % length)
    both = np.stack([np.cos(angle), -np.sin(angle)], axis=1)
    both = both.reshape(width, 2, devices, width // devices).transpose(0, 2, 1, 3)
    forward = both.reshape(width, 2 * width)
    weight = np.where(np.arange(width) == 0, 1.0, 2.0).reshape(devices, 1, width // devices)
    inverse = (both * weight).reshape(width, 2 * width).T / (2.0 * track_freq * length)
    return split_table(forward), split_table(inverse)


def track_tables(cells):
    freq = 2 * cells
    angle = 2.0 * math.pi / freq * (np.arange(cells)[:, None] * np.arange(cells)[None, :] % freq)
    cosine, sine = np.cos(angle), np.sin(angle)
    sine[:, 0] = np.where(np.arange(cells) % 2 == 0, 1.0, -1.0)
    forward = np.concatenate([cosine, sine], axis=1)
    weight = np.where(np.arange(freq) % cells == 0, 1.0, 2.0)[:, None]
    tables = split_table(forward), split_table(forward.T * weight)
    return tuple(deep(table) for table in tables) if cells <= lane_tile else tables


def product(values, table):
    depth, columns = values.shape[1], table.shape[1] // 2
    high = values.astype(bf16)
    low = (values - high.astype(f32)).astype(bf16)
    if table.shape[0] > depth:
        both = jnp.concatenate([high, low], axis=1)
        out = jnp.dot(both, table[...], preferred_element_type=f32)
        return out[:, :columns] + out[:, columns:]
    rows = values.shape[0]
    both = jnp.concatenate([high, low], axis=0)
    if columns <= 2 * lane_tile:
        out = jnp.dot(both, table[...], preferred_element_type=f32)
        return out[:rows, :columns] + (out[rows:, :columns] + out[:rows, columns:])
    first = jnp.dot(both, table[:, :columns], preferred_element_type=f32)
    second = jnp.dot(high, table[:, columns:], preferred_element_type=f32)
    return first[:rows] + first[rows:] + second


def turned(power, parts):
    real, imag = parts
    return ((real, imag), (-imag, real), (-real, -imag), (imag, -real))[power % 4]


def kernel_body(
    grid_y, devices, layers,
    *refs,
):
    hbm_refs, shift_cell, out_ref, loaded, load_sems, rest = (
        refs[:8], refs[8], refs[9], refs[10:18], refs[18], refs[19:]
    )
    next_ref, field_ref = out_ref.at[0], out_ref.at[1]
    magnet_ref, fwd_y, kernel_ref, inv_y, fwd_t, inv_t, material_ref, region_ref = loaded
    loads = [
        pltpu.make_async_copy(source, target, load_sems.at[n])
        for n, (source, target) in enumerate(zip(hbm_refs, loaded))
    ]
    run_step(
        grid_y, devices, layers, loads, shift_cell, material_ref, magnet_ref, region_ref,
        kernel_ref, fwd_y, inv_y, fwd_t, inv_t, next_ref, field_ref, *rest,
    )


def run_step(
    grid_y, devices, layers, loads,
    shift_ref, material_ref, magnet_ref, region_ref, kernel_ref, fwd_y, inv_y, fwd_t, inv_t,
    next_ref, field_ref,
    joined, initial, state, local_field, slope_ref, halo_out, halo_in, spec, table,
    send_a, recv_a, send_b, recv_b, track_hat, track_prod,
    fill_ref, win_sem, halo_sems, a_send_sem, a_recv_sem, b_send_sem, b_recv_sem,
):
    fields, rows, width = state.shape
    half = layers // 2
    freqs = kernel_ref.shape[2]
    track = devices * rows
    block = 2 * freqs
    groups, _, _, padded = send_a.shape
    group_fields = fields // groups
    group_rows = group_fields * block
    me = lax.axis_index("gx") * grid_y + lax.axis_index("gy")

    def device_of(peer):
        return {"gx": peer // grid_y, "gy": lax.rem(peer, grid_y)}

    def peer_at(offset):
        return lax.rem(me + offset, devices)

    right, left = peer_at(1), peer_at(devices - 1)
    grid_x = devices // grid_y
    my_x, my_y = lax.axis_index("gx"), lax.axis_index("gy")
    rings = []
    for k in range(1, grid_y):
        step_y = jnp.where(my_y < grid_y // 2, k, grid_y - k)
        rings.append(lax.rem(my_y + step_y, grid_y))
    turns = [lax.rem(my_x + a, grid_x) for a in range(grid_x - 1, -1, -1)]
    others = [(far_x, my_y) for far_x in turns[:-1]]
    others += [(far_x, far_y) for far_x in turns for far_y in rings]

    barrier = pltpu.get_barrier_semaphore()
    for far_x, far_y in others[::-1]:
        pl.semaphore_signal(barrier, inc=1, device_id={"gx": far_x, "gy": far_y})
    for load in loads:
        load.start()

    lane_small = lax.broadcasted_iota(jnp.int32, (rows, lane_tile), 1)

    def place(c, sign, z):
        return ((sign ^ (c == 2)) * 3 + c) * half + z

    tiles_all = padded // lane_tile
    cut_a = -(-3 * half * block // lane_tile)
    cut_b = 3 * half * block // lane_tile
    parts_a = [part for part in ((0, cut_a), (cut_a, tiles_all)) if part[0] < part[1]]
    parts_b = [part for part in ((0, cut_b), (cut_b, tiles_all)) if part[0] < part[1]]

    def lanes(part):
        return pl.ds(part[0] * lane_tile, (part[1] - part[0]) * lane_tile)

    def in_block(start):
        return (lane_small >= start) & (lane_small < start + block)

    def halo_copies(step):
        return [
            pltpu.make_async_remote_copy(
                src_ref=halo_out.at[side], dst_ref=halo_in.at[lax.rem(step, 2), 1 - side],
                send_sem=halo_sems.at[lax.rem(step, 2), 0, side],
                recv_sem=halo_sems.at[lax.rem(step, 2), 1, 1 - side],
                device_id=device_of(peer),
            )
            for side, peer in ((0, left), (1, right))
        ]

    def exchange(source, target, send_sem, recv_sem, parts, n, other):
        peer = other[0] * grid_y + other[1]
        return pltpu.make_async_remote_copy(
            src_ref=source.at[0, peer, :, lanes(parts[n])],
            dst_ref=target.at[0, me, :, lanes(parts[n])],
            send_sem=send_sem.at[n], recv_sem=recv_sem.at[n],
            device_id={"gx": other[0], "gy": other[1]},
        )

    def all_blocks(source, target, send_sem, recv_sem, parts, n):
        others = pl.ds(0, devices - 1)
        return pltpu.make_async_remote_copy(
            src_ref=source.at[0, others, :, lanes(parts[n])],
            dst_ref=target.at[0, others, :, lanes(parts[n])],
            send_sem=send_sem.at[n], recv_sem=recv_sem.at[n],
            device_id=device_of(right),
        )

    a_refs = (send_a, recv_a, a_send_sem, a_recv_sem, parts_a)
    b_refs = (send_b, recv_b, b_send_sem, b_recv_sem, parts_b)

    slots = lane_tile // block
    spread = freqs % 8 == 0
    my_slot = lax.rem(me, slots)

    def slot_of(turn, f):
        return (turn + f) % slots if spread else f % slots

    def width_blocks(values, target, parts, send):
        spec[...] = product(jnp.concatenate(values, axis=0), fwd_y)
        for n, part in enumerate(parts):
            for j in range(devices // slots):
                pieces = {}

                def turned_piece(f, amount):
                    if (f, amount) not in pieces:
                        piece = spec[pl.ds(f * rows, rows), pl.ds(j * lane_tile, lane_tile)]
                        pieces[f, amount] = pltpu.roll(piece, amount, 1) if amount else piece
                    return pieces[f, amount]

                for turn in range(slots):
                    for t in range(*part):
                        value = jnp.zeros((rows, lane_tile), f32)
                        for k, f in enumerate(range(t * slots, min((t + 1) * slots, fields))):
                            slot = slot_of(turn, f)
                            piece = turned_piece(f, (slot - turn) % slots * block)
                            full = k == 0 and fields - f >= slots
                            value = piece if full else jnp.where(in_block(slot * block), piece, value)
                        target[0, j * slots + turn, :, pl.ds(t * lane_tile, lane_tile)] = value
            send(n)

    def mirrored(cells):
        values = [None] * fields
        for c in range(3):
            for z in range(half):
                a, b = cells[c * layers + z], cells[c * layers + layers - 1 - z]
                values[place(c, 0, z)] = a + b
                values[place(c, 1, z)] = a - b
        return values

    def send_forward(n):
        for o in others:
            exchange(*a_refs, n, o).start()
        if n == len(parts_a) - 1:
            recv_a[0, me] = send_a[0, me]

    def send_first(n):
        if n == 0:
            pl.semaphore_wait(barrier, devices - 1)
        send_forward(n)

    for load in loads[:2]:
        load.wait()
    width_blocks(mirrored(magnet_ref), send_a, parts_a, send_first)
    window_copy = pltpu.make_async_remote_copy(
        src_ref=magnet_ref, dst_ref=joined.at[:, pl.ds(rows, rows)],
        send_sem=win_sem.at[0], recv_sem=win_sem.at[1], device_id=device_of(left),
    )
    window_copy.start()

    joined[:, pl.ds(0, rows)] = magnet_ref[...]
    fill_values = [
        jnp.full((rows, width), 2.0 if f // half == 5 else 0.0, f32) for f in range(fields)
    ]
    width_blocks(fill_values, send_b, parts_b, lambda n: None)
    fill_ref[...] = send_b[:, me]
    for load in loads[2:]:
        load.wait()
    lane_track = lax.broadcasted_iota(jnp.int32, (freqs, track), 1)
    for c in range(6):
        for z in range(half):
            for w in range(half):
                near = kernel_ref[c, layers - 1 + z - w]
                far = kernel_ref[c, 2 * layers - 2 - z - w]
                for sign, value in enumerate((near + far, near - far)):
                    cosines = value[:, :track]
                    table[c, z, w, sign, :, pl.ds(0, track)] = cosines
                    table[c, z, w, sign, :, pl.ds(track, track)] = jnp.where(
                        lane_track == 0, value[:, track:], cosines
                    )
    if padded > group_rows:
        track_prod[...] = jnp.zeros_like(track_prod)

    offset = shift_ref[0]
    row_index = lax.broadcasted_iota(jnp.int32, (rows, width), 0)
    lane_index = lax.broadcasted_iota(jnp.int32, (rows, width), 1)
    beyond = track - offset

    def set_window():
        window_copy.wait()
        for f in range(fields):
            fill = 1.0 if f // layers == 2 else 0.0
            moved = pltpu.roll(joined[f], 2 * rows - offset, 0)
            cells = jnp.where(me * rows + row_index >= beyond, fill, moved[:rows])
            initial[f] = cells
            state[f] = cells
            next_ref[f] = cells
            halo_in[0, 0, pl.ds(f, 1), :] = jnp.where(
                me * rows - 1 >= beyond, fill, moved[2 * rows - 1 :]
            )
            halo_in[0, 1, pl.ds(f, 1), :] = jnp.where(
                me * rows + rows >= beyond, fill, moved[rows : rows + 1]
            )

    def stage(step, carry):
        def arrive(n):
            all_blocks(*a_refs, n).wait_recv()
            part = lanes(parts_a[n])

            @pl.when(step == 0)
            def _():
                whole = recv_a[0, :, :, part].reshape(track, part.size)
                moved = pltpu.roll(whole, track - offset, 0)
                cell = lax.broadcasted_iota(jnp.int32, moved.shape, 0)
                moved = jnp.where(cell >= beyond, fill_ref[0, pl.ds(0, 1), part], moved)
                recv_a[0, :, :, part] = moved.reshape(devices, rows, part.size)

            arrived = recv_a[0, :, :, part].reshape(track, part.size)
            track_hat[part] = product(arrived.T, fwd_t)

        def give_back(n):
            part = lanes(parts_b[n])
            back = product(track_prod[part], inv_t).T
            send_b[0, :, :, part] = back.reshape(devices, rows, part.size)
            for o in others:
                exchange(*b_refs, n, o).start()
            recv_b[0, me, :, part] = send_b[0, me, :, part]

        def place_row(c, sign, z):
            f = place(c, sign, z)
            if not spread:
                return f * block
            return f // slots * lane_tile + lax.rem(my_slot + f % slots, slots) * block

        def row_of(first, p, low):
            row = first + p * freqs + low
            return pl.multiple_of(row, 8) if spread else row

        def hat(c, sign, z, odd, low, span):
            first = place_row(c, sign, z)
            return tuple(
                track_hat[pl.ds(row_of(first, p, low), span), pl.ds(odd * track, track)]
                for p in range(2)
            )

        for chosen in range(2):
            if chosen < len(parts_a):
                arrive(chosen)
            span = min(freqs, 8)
            for half_track in range(2):
                for low in range(0, freqs, span):
                    for i in range(3):
                        odd = half_track if i == 0 else 1 - half_track
                        columns = pl.ds(odd * track, track)
                        sign = chosen ^ (i == 2)
                        for z in range(half):
                            total = [None, None]
                            for j in range(3):
                                c = pair_comp[i][j]
                                power = 1 if c >= 4 else 0
                                swap = c in (3, 4)
                                if swap:
                                    power += 1 if odd else 3
                                for w in range(half):
                                    tab = table[c, z, w, sign, pl.ds(low, span), columns]
                                    source = hat(
                                        j, sign ^ (c >= 4), w, 1 - odd if swap else odd, low, span
                                    )
                                    parts = turned(power, tuple(tab * value for value in source))
                                    total = [
                                        part if old is None else old + part
                                        for old, part in zip(total, parts)
                                    ]
                            first = place_row(i, sign, z)
                            for p in range(2):
                                track_prod[pl.ds(row_of(first, p, low), span), columns] = total[p]

            if chosen == 1 or len(parts_b) == 2:
                give_back(min(chosen, len(parts_b) - 1))

        @pl.when(step == 0)
        def _():
            set_window()

        @pl.when(step > 0)
        def _():
            for copy in halo_copies(step):
                copy.wait()

        turn = lax.rem(step, 2)

        flow = region_ref[...].astype(f32)
        for z in range(layers):
            drift = material_ref[z, 4] * flow
            for c in range(3):
                f = c * layers + z
                cells = state[f]
                before = jnp.where(me == 0, cells[0:1], halo_in[turn, 0, pl.ds(f, 1), :])
                after = jnp.where(
                    me == devices - 1, cells[rows - 1 : rows], halo_in[turn, 1, pl.ds(f, 1), :]
                )
                up = jnp.where(row_index == 0, before, pltpu.roll(cells, 1, 0))
                down = jnp.where(row_index == rows - 1, after, pltpu.roll(cells, rows - 1, 0))
                side_a = jnp.where(lane_index == 0, cells, pltpu.roll(cells, 1, 1))
                side_b = jnp.where(
                    lane_index == width - 1, cells, pltpu.roll(cells, width - 1, 1)
                )
                below = state[c * layers + max(z - 1, 0)]
                above = state[c * layers + min(z + 1, layers - 1)]
                laplace = up + down + side_a + side_b + below + above - 6.0 * cells
                effective = material_ref[z, 2] * laplace
                if c == 2:
                    effective = effective + material_ref[z, 3] * cells
                local_field[f] = effective
                slope_ref[f] = drift * (0.5 * (down - up))

        for f in range(fields):
            t = f // slots
            for n, part in enumerate(parts_b):
                if f == t * slots and t == part[0]:
                    if n == len(parts_b) - 1:
                        for refs in (a_refs, b_refs):
                            for m in range(len(refs[-1])):
                                all_blocks(*refs, m).wait_send()
                    all_blocks(*b_refs, n).wait_recv()
            for j in range(devices // slots):
                value = None
                for turn in range(slots):
                    slot = slot_of(turn, f)
                    piece = recv_b[0, j * slots + turn, :, pl.ds(t * lane_tile, lane_tile)]
                    start = slot * block
                    if not spread and slot != turn:
                        piece = pltpu.roll(piece, (turn - slot) % slots * block, 1)
                        start = turn * block
                    elif not spread:
                        start = turn * block
                    value = piece if value is None else jnp.where(in_block(start), piece, value)
                if spread and f % slots:
                    value = pltpu.roll(value, (-f) % slots * block, 1)
                spec[pl.ds(f * rows, rows), pl.ds(j * lane_tile, lane_tile)] = value
        whole_field = product(spec[...], inv_y)
        demag = [whole_field[f * rows : (f + 1) * rows] for f in range(fields)]

        weight = jnp.where((step == 0) | (step == 3), time_step / 6.0, time_step / 3.0)
        ahead = jnp.where(step == 2, time_step, 0.5 * time_step)

        def demag_of(c, sign, z):
            return demag[place(c, sign, z)]

        for z in range(layers):
            mirror = min(z, layers - 1 - z)
            m, h, g = [], [], []
            for c in range(3):
                f = c * layers + z
                even, odd = demag_of(c, 0, mirror), demag_of(c, 1, mirror)
                value = local_field[f] + (even + odd if z < half else even - odd)
                local_field[f] = value
                m.append(state[f])
                h.append(value)
                g.append(slope_ref[f])

            def cross(a, b):
                return [
                    a[1] * b[2] - a[2] * b[1],
                    a[2] * b[0] - a[0] * b[2],
                    a[0] * b[1] - a[1] * b[0],
                ]

            damping = jnp.full((rows, width), material_ref[z, 0], f32)
            adiabatic = material_ref[z, 1]
            scale = 1.0 / (1.0 + damping * damping)
            torque_h, torque_u = cross(m, h), cross(m, g)
            inner = [
                (1.0 + damping * adiabatic) * u - damping * t for t, u in zip(torque_h, torque_u)
            ]
            outer = cross(m, inner)
            for c in range(3):
                f = c * layers + z
                change = (outer[c] - torque_h[c] + (adiabatic - damping) * torque_u[c]) * scale
                next_ref[f] = next_ref[f] + weight * change
                state[f] = initial[f] + ahead * change

        @pl.when(step < 3)
        def _():
            width_blocks(mirrored(state), send_a, parts_a, send_forward)
            for f in range(fields):
                halo_out[0, pl.ds(f, 1), :] = state[f, pl.ds(0, 1), :]
                halo_out[1, pl.ds(f, 1), :] = state[f, pl.ds(rows - 1, 1), :]
            for copy in halo_copies(step + 1):
                copy.start()

        @pl.when(step == 0)
        def _():
            field_ref[...] = local_field[...]

        return carry

    lax.fori_loop(0, 4, stage, 0)


def local(magnet, window_shift, region, material, kernel):
    components, layers, rows, width = magnet.shape
    grid_y = lax.axis_size("gy")
    devices = lax.axis_size("gx") * grid_y
    fields = components * layers
    track = rows * devices
    freqs = kernel.shape[2]
    groups = 1
    padded = -(-fields // groups * 2 * freqs // lane_tile) * lane_tile
    tables = (*width_tables(width, devices, 2 * track), *track_tables(track))
    vmem = pl.BlockSpec(memory_space=pltpu.VMEM)
    cells = (fields, rows, width)
    half = layers // 2
    blocks = (groups, devices, rows, padded)
    out = pltpu.VMEM((2, *cells), f32)
    dma = pltpu.SemaphoreType.DMA
    both = pl.pallas_call(
        functools.partial(kernel_body, grid_y, devices, layers),
        out_shape=out,
        in_specs=[pl.BlockSpec(memory_space=pltpu.HBM)] * 8 + [pl.BlockSpec(memory_space=pltpu.SMEM)],
        out_specs=vmem,
        scratch_shapes=[
            pltpu.VMEM(cells, f32),
            pltpu.VMEM(tables[0].shape, bf16),
            pltpu.VMEM(kernel.shape, f32),
            *[pltpu.VMEM(table.shape, bf16) for table in tables[1:]],
            pltpu.SMEM(material.shape, f32),
            pltpu.VMEM(region.shape, jnp.int32),
            dma((8,)),
            pltpu.VMEM((fields, 2 * rows, width), f32),
            pltpu.VMEM(cells, f32),
            pltpu.VMEM(cells, f32),
            pltpu.VMEM(cells, f32),
            pltpu.VMEM(cells, f32),
            pltpu.VMEM((2, fields, width), f32),
            pltpu.VMEM((2, 2, fields, width), f32),
            pltpu.VMEM((fields // groups * rows, 2 * width), f32),
            pltpu.VMEM((6, half, half, 2, freqs, 2 * track), f32),
            pltpu.VMEM(blocks, f32),
            pltpu.VMEM(blocks, f32),
            pltpu.VMEM(blocks, f32),
            pltpu.VMEM(blocks, f32),
            pltpu.VMEM((groups * padded, 2 * track), f32),
            pltpu.VMEM((groups * padded, 2 * track), f32),
            pltpu.VMEM((groups, rows, padded), f32),
            dma((2,)),
            dma((2, 2, 2)),
            dma((2,)),
            dma((2,)),
            dma((2,)),
            dma((2,)),
        ],
        compiler_params=pltpu.CompilerParams(
            collective_id=0, has_side_effects=True, vmem_limit_bytes=60 * 2**20
        ),
    )(
        magnet.reshape(cells),
        jnp.asarray(tables[0]),
        kernel,
        *[jnp.asarray(table) for table in tables[1:]],
        material,
        region,
        window_shift,
    )
    return both[0].reshape(magnet.shape), both[1].reshape(magnet.shape)


def solution(mesh):
    cells = P(None, None, ("run", "gx", "gy"), None)
    in_specs = (
        cells,
        P("run"),
        P(("run", "gx", "gy"), None),
        P(),
        P(None, None, ("gx", "gy"), None),
    )
    return jax.shard_map(
        local, mesh=mesh, in_specs=in_specs, out_specs=(cells, cells), check_vma=False
    )
```

```python
import functools
import math

import jax
import jax.numpy as jnp
import numpy as np
from jax import lax
from jax.experimental import pallas as pl
from jax.experimental.pallas import tpu as pltpu
from jax.sharding import PartitionSpec as P

time_step = 0.1
pair_comp = ((0, 3, 4), (3, 1, 5), (4, 5, 2))
lane_tile = 128
f32, bf16 = jnp.float32, jnp.bfloat16


def split_table(table):
    high = table.astype(bf16)
    low = (table - high.astype(np.float64)).astype(bf16)
    return np.concatenate([high, low], axis=1)


def deep(table):
    return np.concatenate([table, table], axis=0)


def width_tables(width, devices, track_freq):
    length = 2 * width - 1
    angle = 2.0 * math.pi / length * (np.arange(width)[:, None] * np.arange(width)[None, :] % length)
    both = np.stack([np.cos(angle), -np.sin(angle)], axis=1)
    both = both.reshape(width, 2, devices, width // devices).transpose(0, 2, 1, 3)
    forward = both.reshape(width, 2 * width)
    weight = np.where(np.arange(width) == 0, 1.0, 2.0).reshape(devices, 1, width // devices)
    inverse = (both * weight).reshape(width, 2 * width).T / (2.0 * track_freq * length)
    return split_table(forward), split_table(inverse)


def track_tables(cells):
    freq = 2 * cells
    angle = 2.0 * math.pi / freq * (np.arange(cells)[:, None] * np.arange(cells)[None, :] % freq)
    cosine, sine = np.cos(angle), np.sin(angle)
    sine[:, 0] = np.where(np.arange(cells) % 2 == 0, 1.0, -1.0)
    forward = np.concatenate([cosine, sine], axis=1)
    weight = np.where(np.arange(freq) % cells == 0, 1.0, 2.0)[:, None]
    tables = split_table(forward), split_table(forward.T * weight)
    return tuple(deep(table) for table in tables) if cells <= lane_tile else tables


def product(values, table):
    depth, columns = values.shape[1], table.shape[1] // 2
    high = values.astype(bf16)
    low = (values - high.astype(f32)).astype(bf16)
    if table.shape[0] > depth:
        both = jnp.concatenate([high, low], axis=1)
        out = jnp.dot(both, table[...], preferred_element_type=f32)
        return out[:, :columns] + out[:, columns:]
    rows = values.shape[0]
    both = jnp.concatenate([high, low], axis=0)
    if columns <= 2 * lane_tile:
        out = jnp.dot(both, table[...], preferred_element_type=f32)
        return out[:rows, :columns] + (out[rows:, :columns] + out[:rows, columns:])
    first = jnp.dot(both, table[:, :columns], preferred_element_type=f32)
    second = jnp.dot(high, table[:, columns:], preferred_element_type=f32)
    return first[:rows] + first[rows:] + second


def turned(power, parts):
    real, imag = parts
    return ((real, imag), (-imag, real), (-real, -imag), (imag, -real))[power % 4]


def kernel_body(
    grid_y, devices, layers,
    *refs,
):
    hbm_refs, shift_cell, out_ref, loaded, load_sems, rest = (
        refs[:8], refs[8], refs[9], refs[10:18], refs[18], refs[19:]
    )
    next_ref, field_ref = out_ref.at[0], out_ref.at[1]
    magnet_ref, fwd_y, kernel_ref, inv_y, fwd_t, inv_t, material_ref, region_ref = loaded
    loads = [
        pltpu.make_async_copy(source, target, load_sems.at[n])
        for n, (source, target) in enumerate(zip(hbm_refs, loaded))
    ]
    run_step(
        grid_y, devices, layers, loads, shift_cell, material_ref, magnet_ref, region_ref,
        kernel_ref, fwd_y, inv_y, fwd_t, inv_t, next_ref, field_ref, *rest,
    )


def run_step(
    grid_y, devices, layers, loads,
    shift_ref, material_ref, magnet_ref, region_ref, kernel_ref, fwd_y, inv_y, fwd_t, inv_t,
    next_ref, field_ref,
    joined, initial, state, local_field, slope_ref, halo_out, halo_in, spec, table,
    send_a, recv_a, send_b, recv_b, track_hat, track_prod,
    fill_ref, win_sem, halo_sems, a_send_sem, a_recv_sem, b_send_sem, b_recv_sem,
):
    fields, rows, width = state.shape
    half = layers // 2
    freqs = kernel_ref.shape[2]
    track = devices * rows
    block = 2 * freqs
    groups, _, _, padded = send_a.shape
    group_fields = fields // groups
    group_rows = group_fields * block
    me = lax.axis_index("gx") * grid_y + lax.axis_index("gy")

    def device_of(peer):
        return {"gx": peer // grid_y, "gy": lax.rem(peer, grid_y)}

    def peer_at(offset):
        return lax.rem(me + offset, devices)

    right, left = peer_at(1), peer_at(devices - 1)
    grid_x = devices // grid_y
    my_x, my_y = lax.axis_index("gx"), lax.axis_index("gy")
    rings = []
    for k in range(1, grid_y):
        step_y = jnp.where(my_y < grid_y // 2, k, grid_y - k)
        rings.append(lax.rem(my_y + step_y, grid_y))
    turns = [lax.rem(my_x + a, grid_x) for a in range(grid_x - 1, -1, -1)]
    others = [(far_x, my_y) for far_x in turns[:-1]]
    others += [(far_x, far_y) for far_x in turns for far_y in rings]

    barrier = pltpu.get_barrier_semaphore()
    for far_x, far_y in others[::-1]:
        pl.semaphore_signal(barrier, inc=1, device_id={"gx": far_x, "gy": far_y})
    for load in loads:
        load.start()

    lane_small = lax.broadcasted_iota(jnp.int32, (rows, lane_tile), 1)

    def place(c, sign, z):
        return ((sign ^ (c == 2)) * 3 + c) * half + z

    tiles_all = padded // lane_tile
    cut_a = -(-3 * half * block // lane_tile)
    cut_b = 3 * half * block // lane_tile
    parts_a = [part for part in ((0, cut_a), (cut_a, tiles_all)) if part[0] < part[1]]
    parts_b = [part for part in ((0, cut_b), (cut_b, tiles_all)) if part[0] < part[1]]

    def lanes(part):
        return pl.ds(part[0] * lane_tile, (part[1] - part[0]) * lane_tile)

    def in_block(start):
        return (lane_small >= start) & (lane_small < start + block)

    def halo_copies(step):
        return [
            pltpu.make_async_remote_copy(
                src_ref=halo_out.at[side], dst_ref=halo_in.at[lax.rem(step, 2), 1 - side],
                send_sem=halo_sems.at[lax.rem(step, 2), 0, side],
                recv_sem=halo_sems.at[lax.rem(step, 2), 1, 1 - side],
                device_id=device_of(peer),
            )
            for side, peer in ((0, left), (1, right))
        ]

    def exchange(source, target, send_sem, recv_sem, parts, n, other):
        peer = other[0] * grid_y + other[1]
        return pltpu.make_async_remote_copy(
            src_ref=source.at[0, peer, :, lanes(parts[n])],
            dst_ref=target.at[0, me, :, lanes(parts[n])],
            send_sem=send_sem.at[n], recv_sem=recv_sem.at[n],
            device_id={"gx": other[0], "gy": other[1]},
        )

    def all_blocks(source, target, send_sem, recv_sem, parts, n):
        others = pl.ds(0, devices - 1)
        return pltpu.make_async_remote_copy(
            src_ref=source.at[0, others, :, lanes(parts[n])],
            dst_ref=target.at[0, others, :, lanes(parts[n])],
            send_sem=send_sem.at[n], recv_sem=recv_sem.at[n],
            device_id=device_of(right),
        )

    a_refs = (send_a, recv_a, a_send_sem, a_recv_sem, parts_a)
    b_refs = (send_b, recv_b, b_send_sem, b_recv_sem, parts_b)

    slots = lane_tile // block
    spread = freqs % 8 == 0
    my_slot = lax.rem(me, slots)

    def slot_of(turn, f):
        return (turn + f) % slots if spread else f % slots

    def width_blocks(values, target, parts, send):
        spec[...] = product(jnp.concatenate(values, axis=0), fwd_y)
        for n, part in enumerate(parts):
            for j in range(devices // slots):
                pieces = {}

                def turned_piece(f, amount):
                    if (f, amount) not in pieces:
                        piece = spec[pl.ds(f * rows, rows), pl.ds(j * lane_tile, lane_tile)]
                        pieces[f, amount] = pltpu.roll(piece, amount, 1) if amount else piece
                    return pieces[f, amount]

                for turn in range(slots):
                    for t in range(*part):
                        value = jnp.zeros((rows, lane_tile), f32)
                        for k, f in enumerate(range(t * slots, min((t + 1) * slots, fields))):
                            slot = slot_of(turn, f)
                            piece = turned_piece(f, (slot - turn) % slots * block)
                            full = k == 0 and fields - f >= slots
                            value = piece if full else jnp.where(in_block(slot * block), piece, value)
                        target[0, j * slots + turn, :, pl.ds(t * lane_tile, lane_tile)] = value
            send(n)

    def mirrored(cells):
        values = [None] * fields
        for c in range(3):
            for z in range(half):
                a, b = cells[c * layers + z], cells[c * layers + layers - 1 - z]
                values[place(c, 0, z)] = a + b
                values[place(c, 1, z)] = a - b
        return values

    def send_forward(n):
        for o in others:
            exchange(*a_refs, n, o).start()
        if n == len(parts_a) - 1:
            recv_a[0, me] = send_a[0, me]

    def send_first(n):
        if n == 0:
            pl.semaphore_wait(barrier, devices - 1)
        send_forward(n)

    for load in loads[:2]:
        load.wait()
    width_blocks(mirrored(magnet_ref), send_a, parts_a, send_first)
    window_copy = pltpu.make_async_remote_copy(
        src_ref=magnet_ref, dst_ref=joined.at[:, pl.ds(rows, rows)],
        send_sem=win_sem.at[0], recv_sem=win_sem.at[1], device_id=device_of(left),
    )
    window_copy.start()

    joined[:, pl.ds(0, rows)] = magnet_ref[...]
    fill_values = [
        jnp.full((rows, width), 2.0 if f // half == 5 else 0.0, f32) for f in range(fields)
    ]
    width_blocks(fill_values, send_b, parts_b, lambda n: None)
    fill_ref[...] = send_b[:, me]
    for load in loads[2:]:
        load.wait()
    lane_track = lax.broadcasted_iota(jnp.int32, (freqs, track), 1)
    for c in range(6):
        for z in range(half):
            for w in range(half):
                near = kernel_ref[c, layers - 1 + z - w]
                far = kernel_ref[c, 2 * layers - 2 - z - w]
                for sign, value in enumerate((near + far, near - far)):
                    cosines = value[:, :track]
                    table[c, z, w, sign, :, pl.ds(0, track)] = cosines
                    table[c, z, w, sign, :, pl.ds(track, track)] = jnp.where(
                        lane_track == 0, value[:, track:], cosines
                    )
    if padded > group_rows:
        track_prod[...] = jnp.zeros_like(track_prod)

    offset = shift_ref[0]
    row_index = lax.broadcasted_iota(jnp.int32, (rows, width), 0)
    lane_index = lax.broadcasted_iota(jnp.int32, (rows, width), 1)
    beyond = track - offset

    def set_window():
        window_copy.wait()
        for f in range(fields):
            fill = 1.0 if f // layers == 2 else 0.0
            moved = pltpu.roll(joined[f], 2 * rows - offset, 0)
            cells = jnp.where(me * rows + row_index >= beyond, fill, moved[:rows])
            initial[f] = cells
            state[f] = cells
            next_ref[f] = cells
            halo_in[0, 0, pl.ds(f, 1), :] = jnp.where(
                me * rows - 1 >= beyond, fill, moved[2 * rows - 1 :]
            )
            halo_in[0, 1, pl.ds(f, 1), :] = jnp.where(
                me * rows + rows >= beyond, fill, moved[rows : rows + 1]
            )

    def stage(step, carry):
        def arrive(n):
            all_blocks(*a_refs, n).wait_recv()
            part = lanes(parts_a[n])

            @pl.when(step == 0)
            def _():
                whole = recv_a[0, :, :, part].reshape(track, part.size)
                moved = pltpu.roll(whole, track - offset, 0)
                cell = lax.broadcasted_iota(jnp.int32, moved.shape, 0)
                moved = jnp.where(cell >= beyond, fill_ref[0, pl.ds(0, 1), part], moved)
                recv_a[0, :, :, part] = moved.reshape(devices, rows, part.size)

            for t in range(*parts_a[n]):
                tile = pl.ds(t * lane_tile, lane_tile)
                arrived = recv_a[0, :, :, tile].reshape(track, lane_tile)
                track_hat[tile] = product(arrived.T, fwd_t)

        def give_back(n):
            part = lanes(parts_b[n])
            for t in range(*parts_b[n]):
                tile = pl.ds(t * lane_tile, lane_tile)
                back = product(track_prod[tile], inv_t).T
                send_b[0, :, :, tile] = back.reshape(devices, rows, lane_tile)
            for o in others:
                exchange(*b_refs, n, o).start()
            recv_b[0, me, :, part] = send_b[0, me, :, part]

        def place_row(c, sign, z):
            f = place(c, sign, z)
            if not spread:
                return f * block
            return f // slots * lane_tile + lax.rem(my_slot + f % slots, slots) * block

        def row_of(first, p, low):
            row = first + p * freqs + low
            return pl.multiple_of(row, 8) if spread else row

        def hat(c, sign, z, odd, low, span):
            first = place_row(c, sign, z)
            return tuple(
                track_hat[pl.ds(row_of(first, p, low), span), pl.ds(odd * track, track)]
                for p in range(2)
            )

        for chosen in range(2):
            if chosen < len(parts_a):
                arrive(chosen)
            span = min(freqs, 8)
            for half_track in range(2):
                for low in range(0, freqs, span):
                    for i in range(3):
                        odd = half_track if i == 0 else 1 - half_track
                        columns = pl.ds(odd * track, track)
                        sign = chosen ^ (i == 2)
                        for z in range(half):
                            total = [None, None]
                            for j in range(3):
                                c = pair_comp[i][j]
                                power = 1 if c >= 4 else 0
                                swap = c in (3, 4)
                                if swap:
                                    power += 1 if odd else 3
                                for w in range(half):
                                    tab = table[c, z, w, sign, pl.ds(low, span), columns]
                                    source = hat(
                                        j, sign ^ (c >= 4), w, 1 - odd if swap else odd, low, span
                                    )
                                    parts = turned(power, tuple(tab * value for value in source))
                                    total = [
                                        part if old is None else old + part
                                        for old, part in zip(total, parts)
                                    ]
                            first = place_row(i, sign, z)
                            for p in range(2):
                                track_prod[pl.ds(row_of(first, p, low), span), columns] = total[p]

            if chosen == 1 or len(parts_b) == 2:
                give_back(min(chosen, len(parts_b) - 1))

        @pl.when(step == 0)
        def _():
            set_window()

        @pl.when(step > 0)
        def _():
            for copy in halo_copies(step):
                copy.wait()

        turn = lax.rem(step, 2)

        flow = region_ref[...].astype(f32)
        for z in range(layers):
            drift = material_ref[z, 4] * flow
            for c in range(3):
                f = c * layers + z
                cells = state[f]
                before = jnp.where(me == 0, cells[0:1], halo_in[turn, 0, pl.ds(f, 1), :])
                after = jnp.where(
                    me == devices - 1, cells[rows - 1 : rows], halo_in[turn, 1, pl.ds(f, 1), :]
                )
                up = jnp.where(row_index == 0, before, pltpu.roll(cells, 1, 0))
                down = jnp.where(row_index == rows - 1, after, pltpu.roll(cells, rows - 1, 0))
                side_a = jnp.where(lane_index == 0, cells, pltpu.roll(cells, 1, 1))
                side_b = jnp.where(
                    lane_index == width - 1, cells, pltpu.roll(cells, width - 1, 1)
                )
                below = state[c * layers + max(z - 1, 0)]
                above = state[c * layers + min(z + 1, layers - 1)]
                laplace = up + down + side_a + side_b + below + above - 6.0 * cells
                effective = material_ref[z, 2] * laplace
                if c == 2:
                    effective = effective + material_ref[z, 3] * cells
                local_field[f] = effective
                slope_ref[f] = drift * (0.5 * (down - up))

        for f in range(fields):
            t = f // slots
            for n, part in enumerate(parts_b):
                if f == t * slots and t == part[0]:
                    if n == len(parts_b) - 1:
                        for refs in (a_refs, b_refs):
                            for m in range(len(refs[-1])):
                                all_blocks(*refs, m).wait_send()
                    all_blocks(*b_refs, n).wait_recv()
            for j in range(devices // slots):
                value = None
                for turn in range(slots):
                    slot = slot_of(turn, f)
                    piece = recv_b[0, j * slots + turn, :, pl.ds(t * lane_tile, lane_tile)]
                    start = slot * block
                    if not spread and slot != turn:
                        piece = pltpu.roll(piece, (turn - slot) % slots * block, 1)
                        start = turn * block
                    elif not spread:
                        start = turn * block
                    value = piece if value is None else jnp.where(in_block(start), piece, value)
                if spread and f % slots:
                    value = pltpu.roll(value, (-f) % slots * block, 1)
                spec[pl.ds(f * rows, rows), pl.ds(j * lane_tile, lane_tile)] = value
        whole_field = product(spec[...], inv_y)
        demag = [whole_field[f * rows : (f + 1) * rows] for f in range(fields)]

        weight = jnp.where((step == 0) | (step == 3), time_step / 6.0, time_step / 3.0)
        ahead = jnp.where(step == 2, time_step, 0.5 * time_step)

        def demag_of(c, sign, z):
            return demag[place(c, sign, z)]

        for z in range(layers):
            mirror = min(z, layers - 1 - z)
            m, h, g = [], [], []
            for c in range(3):
                f = c * layers + z
                even, odd = demag_of(c, 0, mirror), demag_of(c, 1, mirror)
                value = local_field[f] + (even + odd if z < half else even - odd)
                local_field[f] = value
                m.append(state[f])
                h.append(value)
                g.append(slope_ref[f])

            def cross(a, b):
                return [
                    a[1] * b[2] - a[2] * b[1],
                    a[2] * b[0] - a[0] * b[2],
                    a[0] * b[1] - a[1] * b[0],
                ]

            damping = jnp.full((rows, width), material_ref[z, 0], f32)
            adiabatic = material_ref[z, 1]
            scale = 1.0 / (1.0 + damping * damping)
            torque_h, torque_u = cross(m, h), cross(m, g)
            inner = [
                (1.0 + damping * adiabatic) * u - damping * t for t, u in zip(torque_h, torque_u)
            ]
            outer = cross(m, inner)
            for c in range(3):
                f = c * layers + z
                change = (outer[c] - torque_h[c] + (adiabatic - damping) * torque_u[c]) * scale
                next_ref[f] = next_ref[f] + weight * change
                state[f] = initial[f] + ahead * change

        @pl.when(step < 3)
        def _():
            width_blocks(mirrored(state), send_a, parts_a, send_forward)
            for f in range(fields):
                halo_out[0, pl.ds(f, 1), :] = state[f, pl.ds(0, 1), :]
                halo_out[1, pl.ds(f, 1), :] = state[f, pl.ds(rows - 1, 1), :]
            for copy in halo_copies(step + 1):
                copy.start()

        @pl.when(step == 0)
        def _():
            field_ref[...] = local_field[...]

        return carry

    lax.fori_loop(0, 4, stage, 0)


def local(magnet, window_shift, region, material, kernel):
    components, layers, rows, width = magnet.shape
    grid_y = lax.axis_size("gy")
    devices = lax.axis_size("gx") * grid_y
    fields = components * layers
    track = rows * devices
    freqs = kernel.shape[2]
    groups = 1
    padded = -(-fields // groups * 2 * freqs // lane_tile) * lane_tile
    tables = (*width_tables(width, devices, 2 * track), *track_tables(track))
    vmem = pl.BlockSpec(memory_space=pltpu.VMEM)
    cells = (fields, rows, width)
    half = layers // 2
    blocks = (groups, devices, rows, padded)
    out = pltpu.VMEM((2, *cells), f32)
    dma = pltpu.SemaphoreType.DMA
    both = pl.pallas_call(
        functools.partial(kernel_body, grid_y, devices, layers),
        out_shape=out,
        in_specs=[pl.BlockSpec(memory_space=pltpu.HBM)] * 8 + [pl.BlockSpec(memory_space=pltpu.SMEM)],
        out_specs=vmem,
        scratch_shapes=[
            pltpu.VMEM(cells, f32),
            pltpu.VMEM(tables[0].shape, bf16),
            pltpu.VMEM(kernel.shape, f32),
            *[pltpu.VMEM(table.shape, bf16) for table in tables[1:]],
            pltpu.SMEM(material.shape, f32),
            pltpu.VMEM(region.shape, jnp.int32),
            dma((8,)),
            pltpu.VMEM((fields, 2 * rows, width), f32),
            pltpu.VMEM(cells, f32),
            pltpu.VMEM(cells, f32),
            pltpu.VMEM(cells, f32),
            pltpu.VMEM(cells, f32),
            pltpu.VMEM((2, fields, width), f32),
            pltpu.VMEM((2, 2, fields, width), f32),
            pltpu.VMEM((fields // groups * rows, 2 * width), f32),
            pltpu.VMEM((6, half, half, 2, freqs, 2 * track), f32),
            pltpu.VMEM(blocks, f32),
            pltpu.VMEM(blocks, f32),
            pltpu.VMEM(blocks, f32),
            pltpu.VMEM(blocks, f32),
            pltpu.VMEM((groups * padded, 2 * track), f32),
            pltpu.VMEM((groups * padded, 2 * track), f32),
            pltpu.VMEM((groups, rows, padded), f32),
            dma((2,)),
            dma((2, 2, 2)),
            dma((2,)),
            dma((2,)),
            dma((2,)),
            dma((2,)),
        ],
        compiler_params=pltpu.CompilerParams(
            collective_id=0, has_side_effects=True, vmem_limit_bytes=60 * 2**20
        ),
    )(
        magnet.reshape(cells),
        jnp.asarray(tables[0]),
        kernel,
        *[jnp.asarray(table) for table in tables[1:]],
        material,
        region,
        window_shift,
    )
    return both[0].reshape(magnet.shape), both[1].reshape(magnet.shape)


def solution(mesh):
    cells = P(None, None, ("run", "gx", "gy"), None)
    in_specs = (
        cells,
        P("run"),
        P(("run", "gx", "gy"), None),
        P(),
        P(None, None, ("gx", "gy"), None),
    )
    return jax.shard_map(
        local, mesh=mesh, in_specs=in_specs, out_specs=(cells, cells), check_vma=False
    )
```

```python
import functools
import math

import jax
import jax.numpy as jnp
import numpy as np
from jax import lax
from jax.experimental import pallas as pl
from jax.experimental.pallas import tpu as pltpu
from jax.sharding import PartitionSpec as P

time_step = 0.1
pair_comp = ((0, 3, 4), (3, 1, 5), (4, 5, 2))
lane_tile = 128
f32, bf16 = jnp.float32, jnp.bfloat16


def split_table(table):
    high = table.astype(bf16)
    low = (table - high.astype(np.float64)).astype(bf16)
    return np.concatenate([high, low], axis=1)


def deep(table):
    return np.concatenate([table, table], axis=0)


def width_tables(width, devices, track_freq):
    length = 2 * width - 1
    angle = 2.0 * math.pi / length * (np.arange(width)[:, None] * np.arange(width)[None, :] % length)
    both = np.stack([np.cos(angle), -np.sin(angle)], axis=1)
    both = both.reshape(width, 2, devices, width // devices).transpose(0, 2, 1, 3)
    forward = both.reshape(width, 2 * width)
    weight = np.where(np.arange(width) == 0, 1.0, 2.0).reshape(devices, 1, width // devices)
    inverse = (both * weight).reshape(width, 2 * width).T / (2.0 * track_freq * length)
    return split_table(forward), split_table(inverse)


def track_tables(cells):
    freq = 2 * cells
    angle = 2.0 * math.pi / freq * (np.arange(cells)[:, None] * np.arange(cells)[None, :] % freq)
    cosine, sine = np.cos(angle), np.sin(angle)
    sine[:, 0] = np.where(np.arange(cells) % 2 == 0, 1.0, -1.0)
    forward = np.concatenate([cosine, sine], axis=1)
    weight = np.where(np.arange(freq) % cells == 0, 1.0, 2.0)[:, None]
    tables = split_table(forward), split_table(forward.T * weight)
    return tuple(deep(table) for table in tables) if cells <= lane_tile else tables


def product(values, table):
    depth, columns = values.shape[1], table.shape[1] // 2
    high = values.astype(bf16)
    low = (values - high.astype(f32)).astype(bf16)
    if table.shape[0] > depth:
        both = jnp.concatenate([high, low], axis=1)
        out = jnp.dot(both, table[...], preferred_element_type=f32)
        return out[:, :columns] + out[:, columns:]
    rows = values.shape[0]
    both = jnp.concatenate([high, low], axis=0)
    if columns <= 2 * lane_tile:
        out = jnp.dot(both, table[...], preferred_element_type=f32)
        return out[:rows, :columns] + (out[rows:, :columns] + out[:rows, columns:])
    first = jnp.dot(both, table[:, :columns], preferred_element_type=f32)
    second = jnp.dot(high, table[:, columns:], preferred_element_type=f32)
    return first[:rows] + first[rows:] + second


def turned(power, parts):
    real, imag = parts
    return ((real, imag), (-imag, real), (-real, -imag), (imag, -real))[power % 4]


def kernel_body(
    grid_y, devices, layers,
    *refs,
):
    hbm_refs, shift_cell, out_ref, loaded, load_sems, rest = (
        refs[:8], refs[8], refs[9], refs[10:18], refs[18], refs[19:]
    )
    next_ref, field_ref = out_ref.at[0], out_ref.at[1]
    magnet_ref, fwd_y, kernel_ref, inv_y, fwd_t, inv_t, material_ref, region_ref = loaded
    loads = [
        pltpu.make_async_copy(source, target, load_sems.at[n])
        for n, (source, target) in enumerate(zip(hbm_refs, loaded))
    ]
    run_step(
        grid_y, devices, layers, loads, shift_cell, material_ref, magnet_ref, region_ref,
        kernel_ref, fwd_y, inv_y, fwd_t, inv_t, next_ref, field_ref, *rest,
    )


def run_step(
    grid_y, devices, layers, loads,
    shift_ref, material_ref, magnet_ref, region_ref, kernel_ref, fwd_y, inv_y, fwd_t, inv_t,
    next_ref, field_ref,
    joined, initial, state, local_field, slope_ref, halo_out, halo_in, spec, table,
    send_a, recv_a, send_b, recv_b, track_hat, track_prod,
    fill_ref, win_sem, halo_sems, a_send_sem, a_recv_sem, b_send_sem, b_recv_sem,
):
    fields, rows, width = state.shape
    half = layers // 2
    freqs = kernel_ref.shape[2]
    track = devices * rows
    block = 2 * freqs
    groups, _, _, padded = send_a.shape
    group_fields = fields // groups
    group_rows = group_fields * block
    me = lax.axis_index("gx") * grid_y + lax.axis_index("gy")

    def device_of(peer):
        return {"gx": peer // grid_y, "gy": lax.rem(peer, grid_y)}

    def peer_at(offset):
        return lax.rem(me + offset, devices)

    right, left = peer_at(1), peer_at(devices - 1)
    grid_x = devices // grid_y
    my_x, my_y = lax.axis_index("gx"), lax.axis_index("gy")
    rings = []
    for k in range(1, grid_y):
        step_y = jnp.where(my_y < grid_y // 2, k, grid_y - k)
        rings.append(lax.rem(my_y + step_y, grid_y))
    turns = [lax.rem(my_x + a, grid_x) for a in range(grid_x - 1, -1, -1)]
    others = [(far_x, my_y) for far_x in turns[:-1]]
    others += [(far_x, far_y) for far_x in turns for far_y in rings]

    for load in loads[:2]:
        load.start()
    barrier = pltpu.get_barrier_semaphore()
    for far_x, far_y in others[::-1]:
        pl.semaphore_signal(barrier, inc=1, device_id={"gx": far_x, "gy": far_y})
    for load in loads[2:]:
        load.start()

    lane_small = lax.broadcasted_iota(jnp.int32, (rows, lane_tile), 1)

    def place(c, sign, z):
        return ((sign ^ (c == 2)) * 3 + c) * half + z

    tiles_all = padded // lane_tile
    cut_a = -(-3 * half * block // lane_tile)
    cut_b = 3 * half * block // lane_tile
    parts_a = [(0, tiles_all)]
    parts_b = [part for part in ((0, cut_b), (cut_b, tiles_all)) if part[0] < part[1]]

    def lanes(part):
        return pl.ds(part[0] * lane_tile, (part[1] - part[0]) * lane_tile)

    def in_block(start):
        return (lane_small >= start) & (lane_small < start + block)

    def halo_copies(step):
        return [
            pltpu.make_async_remote_copy(
                src_ref=halo_out.at[side], dst_ref=halo_in.at[lax.rem(step, 2), 1 - side],
                send_sem=halo_sems.at[lax.rem(step, 2), 0, side],
                recv_sem=halo_sems.at[lax.rem(step, 2), 1, 1 - side],
                device_id=device_of(peer),
            )
            for side, peer in ((0, left), (1, right))
        ]

    def exchange(source, target, send_sem, recv_sem, parts, n, other):
        peer = other[0] * grid_y + other[1]
        return pltpu.make_async_remote_copy(
            src_ref=source.at[0, peer, :, lanes(parts[n])],
            dst_ref=target.at[0, me, :, lanes(parts[n])],
            send_sem=send_sem.at[n], recv_sem=recv_sem.at[n],
            device_id={"gx": other[0], "gy": other[1]},
        )

    def all_blocks(source, target, send_sem, recv_sem, parts, n):
        others = pl.ds(0, devices - 1)
        return pltpu.make_async_remote_copy(
            src_ref=source.at[0, others, :, lanes(parts[n])],
            dst_ref=target.at[0, others, :, lanes(parts[n])],
            send_sem=send_sem.at[n], recv_sem=recv_sem.at[n],
            device_id=device_of(right),
        )

    a_refs = (send_a, recv_a, a_send_sem, a_recv_sem, parts_a)
    b_refs = (send_b, recv_b, b_send_sem, b_recv_sem, parts_b)

    slots = lane_tile // block
    spread = freqs % 8 == 0
    my_slot = lax.rem(me, slots)

    def slot_of(turn, f):
        return (turn + f) % slots if spread else f % slots

    def width_blocks(values, target, parts, send):
        spec[...] = product(jnp.concatenate(values, axis=0), fwd_y)
        for n, part in enumerate(parts):
            for j in range(devices // slots):
                pieces = {}

                def turned_piece(f, amount):
                    if (f, amount) not in pieces:
                        piece = spec[pl.ds(f * rows, rows), pl.ds(j * lane_tile, lane_tile)]
                        pieces[f, amount] = pltpu.roll(piece, amount, 1) if amount else piece
                    return pieces[f, amount]

                for turn in range(slots):
                    for t in range(*part):
                        value = jnp.zeros((rows, lane_tile), f32)
                        for k, f in enumerate(range(t * slots, min((t + 1) * slots, fields))):
                            slot = slot_of(turn, f)
                            piece = turned_piece(f, (slot - turn) % slots * block)
                            full = k == 0 and fields - f >= slots
                            value = piece if full else jnp.where(in_block(slot * block), piece, value)
                        target[0, j * slots + turn, :, pl.ds(t * lane_tile, lane_tile)] = value
            send(n)

    def mirrored(cells):
        values = [None] * fields
        for c in range(3):
            for z in range(half):
                a, b = cells[c * layers + z], cells[c * layers + layers - 1 - z]
                values[place(c, 0, z)] = a + b
                values[place(c, 1, z)] = a - b
        return values

    def send_forward(n):
        for o in others:
            exchange(*a_refs, n, o).start()
        if n == len(parts_a) - 1:
            recv_a[0, me] = send_a[0, me]

    def send_first(n):
        if n == 0:
            pl.semaphore_wait(barrier, devices - 1)
        send_forward(n)

    for load in loads[:2]:
        load.wait()
    width_blocks(mirrored(magnet_ref), send_a, parts_a, send_first)
    window_copy = pltpu.make_async_remote_copy(
        src_ref=magnet_ref, dst_ref=joined.at[:, pl.ds(rows, rows)],
        send_sem=win_sem.at[0], recv_sem=win_sem.at[1], device_id=device_of(left),
    )
    window_copy.start()

    joined[:, pl.ds(0, rows)] = magnet_ref[...]
    fill_values = [
        jnp.full((rows, width), 2.0 if f // half == 5 else 0.0, f32) for f in range(fields)
    ]
    width_blocks(fill_values, send_b, parts_b, lambda n: None)
    fill_ref[...] = send_b[:, me]
    for load in loads[2:]:
        load.wait()
    lane_track = lax.broadcasted_iota(jnp.int32, (freqs, track), 1)
    for c in range(6):
        for z in range(half):
            for w in range(half):
                near = kernel_ref[c, layers - 1 + z - w]
                far = kernel_ref[c, 2 * layers - 2 - z - w]
                for sign, value in enumerate((near + far, near - far)):
                    cosines = value[:, :track]
                    table[c, z, w, sign, :, pl.ds(0, track)] = cosines
                    table[c, z, w, sign, :, pl.ds(track, track)] = jnp.where(
                        lane_track == 0, value[:, track:], cosines
                    )
    if padded > group_rows:
        track_prod[...] = jnp.zeros_like(track_prod)

    offset = shift_ref[0]
    row_index = lax.broadcasted_iota(jnp.int32, (rows, width), 0)
    lane_index = lax.broadcasted_iota(jnp.int32, (rows, width), 1)
    beyond = track - offset

    def set_window():
        window_copy.wait()
        for f in range(fields):
            fill = 1.0 if f // layers == 2 else 0.0
            moved = pltpu.roll(joined[f], 2 * rows - offset, 0)
            cells = jnp.where(me * rows + row_index >= beyond, fill, moved[:rows])
            initial[f] = cells
            state[f] = cells
            next_ref[f] = cells
            halo_in[0, 0, pl.ds(f, 1), :] = jnp.where(
                me * rows - 1 >= beyond, fill, moved[2 * rows - 1 :]
            )
            halo_in[0, 1, pl.ds(f, 1), :] = jnp.where(
                me * rows + rows >= beyond, fill, moved[rows : rows + 1]
            )

    def stage(step, carry):
        def arrive(n):
            all_blocks(*a_refs, n).wait_recv()
            part = lanes(parts_a[n])

            @pl.when(step == 0)
            def _():
                whole = recv_a[0, :, :, part].reshape(track, part.size)
                moved = pltpu.roll(whole, track - offset, 0)
                cell = lax.broadcasted_iota(jnp.int32, moved.shape, 0)
                moved = jnp.where(cell >= beyond, fill_ref[0, pl.ds(0, 1), part], moved)
                recv_a[0, :, :, part] = moved.reshape(devices, rows, part.size)

            for t in range(*parts_a[n]):
                tile = pl.ds(t * lane_tile, lane_tile)
                arrived = recv_a[0, :, :, tile].reshape(track, lane_tile)
                track_hat[tile] = product(arrived.T, fwd_t)

        def give_back(n):
            part = lanes(parts_b[n])
            for t in range(*parts_b[n]):
                tile = pl.ds(t * lane_tile, lane_tile)
                back = product(track_prod[tile], inv_t).T
                send_b[0, :, :, tile] = back.reshape(devices, rows, lane_tile)
            for o in others:
                exchange(*b_refs, n, o).start()
            recv_b[0, me, :, part] = send_b[0, me, :, part]

        def place_row(c, sign, z):
            f = place(c, sign, z)
            if not spread:
                return f * block
            return f // slots * lane_tile + lax.rem(my_slot + f % slots, slots) * block

        def row_of(first, p, low):
            row = first + p * freqs + low
            return pl.multiple_of(row, 8) if spread else row

        def hat(c, sign, z, odd, low, span):
            first = place_row(c, sign, z)
            return tuple(
                track_hat[pl.ds(row_of(first, p, low), span), pl.ds(odd * track, track)]
                for p in range(2)
            )

        for chosen in range(2):
            if chosen < len(parts_a):
                arrive(chosen)
            span = min(freqs, 8)
            for half_track in range(2):
                for low in range(0, freqs, span):
                    for i in range(3):
                        odd = half_track if i == 0 else 1 - half_track
                        columns = pl.ds(odd * track, track)
                        sign = chosen ^ (i == 2)
                        for z in range(half):
                            total = [None, None]
                            for j in range(3):
                                c = pair_comp[i][j]
                                power = 1 if c >= 4 else 0
                                swap = c in (3, 4)
                                if swap:
                                    power += 1 if odd else 3
                                for w in range(half):
                                    tab = table[c, z, w, sign, pl.ds(low, span), columns]
                                    source = hat(
                                        j, sign ^ (c >= 4), w, 1 - odd if swap else odd, low, span
                                    )
                                    parts = turned(power, tuple(tab * value for value in source))
                                    total = [
                                        part if old is None else old + part
                                        for old, part in zip(total, parts)
                                    ]
                            first = place_row(i, sign, z)
                            for p in range(2):
                                track_prod[pl.ds(row_of(first, p, low), span), columns] = total[p]

            if chosen == 1 or len(parts_b) == 2:
                give_back(min(chosen, len(parts_b) - 1))

        @pl.when(step == 0)
        def _():
            set_window()

        @pl.when(step > 0)
        def _():
            for copy in halo_copies(step):
                copy.wait()

        turn = lax.rem(step, 2)

        flow = region_ref[...].astype(f32)
        for z in range(layers):
            drift = material_ref[z, 4] * flow
            for c in range(3):
                f = c * layers + z
                cells = state[f]
                before = jnp.where(me == 0, cells[0:1], halo_in[turn, 0, pl.ds(f, 1), :])
                after = jnp.where(
                    me == devices - 1, cells[rows - 1 : rows], halo_in[turn, 1, pl.ds(f, 1), :]
                )
                up = jnp.where(row_index == 0, before, pltpu.roll(cells, 1, 0))
                down = jnp.where(row_index == rows - 1, after, pltpu.roll(cells, rows - 1, 0))
                side_a = jnp.where(lane_index == 0, cells, pltpu.roll(cells, 1, 1))
                side_b = jnp.where(
                    lane_index == width - 1, cells, pltpu.roll(cells, width - 1, 1)
                )
                below = state[c * layers + max(z - 1, 0)]
                above = state[c * layers + min(z + 1, layers - 1)]
                laplace = up + down + side_a + side_b + below + above - 6.0 * cells
                effective = material_ref[z, 2] * laplace
                if c == 2:
                    effective = effective + material_ref[z, 3] * cells
                local_field[f] = effective
                slope_ref[f] = drift * (0.5 * (down - up))

        for f in range(fields):
            t = f // slots
            for n, part in enumerate(parts_b):
                if f == t * slots and t == part[0]:
                    if n == len(parts_b) - 1:
                        for refs in (a_refs, b_refs):
                            for m in range(len(refs[-1])):
                                all_blocks(*refs, m).wait_send()
                    all_blocks(*b_refs, n).wait_recv()
            for j in range(devices // slots):
                value = None
                for turn in range(slots):
                    slot = slot_of(turn, f)
                    piece = recv_b[0, j * slots + turn, :, pl.ds(t * lane_tile, lane_tile)]
                    start = slot * block
                    if not spread and slot != turn:
                        piece = pltpu.roll(piece, (turn - slot) % slots * block, 1)
                        start = turn * block
                    elif not spread:
                        start = turn * block
                    value = piece if value is None else jnp.where(in_block(start), piece, value)
                if spread and f % slots:
                    value = pltpu.roll(value, (-f) % slots * block, 1)
                spec[pl.ds(f * rows, rows), pl.ds(j * lane_tile, lane_tile)] = value
        whole_field = product(spec[...], inv_y)
        demag = [whole_field[f * rows : (f + 1) * rows] for f in range(fields)]

        weight = jnp.where((step == 0) | (step == 3), time_step / 6.0, time_step / 3.0)
        ahead = jnp.where(step == 2, time_step, 0.5 * time_step)

        def demag_of(c, sign, z):
            return demag[place(c, sign, z)]

        for z in range(layers):
            mirror = min(z, layers - 1 - z)
            m, h, g = [], [], []
            for c in range(3):
                f = c * layers + z
                even, odd = demag_of(c, 0, mirror), demag_of(c, 1, mirror)
                value = local_field[f] + (even + odd if z < half else even - odd)
                local_field[f] = value
                m.append(state[f])
                h.append(value)
                g.append(slope_ref[f])

            def cross(a, b):
                return [
                    a[1] * b[2] - a[2] * b[1],
                    a[2] * b[0] - a[0] * b[2],
                    a[0] * b[1] - a[1] * b[0],
                ]

            damping = jnp.full((rows, width), material_ref[z, 0], f32)
            adiabatic = material_ref[z, 1]
            scale = 1.0 / (1.0 + damping * damping)
            torque_h, torque_u = cross(m, h), cross(m, g)
            inner = [
                (1.0 + damping * adiabatic) * u - damping * t for t, u in zip(torque_h, torque_u)
            ]
            outer = cross(m, inner)
            for c in range(3):
                f = c * layers + z
                change = (outer[c] - torque_h[c] + (adiabatic - damping) * torque_u[c]) * scale
                next_ref[f] = next_ref[f] + weight * change
                state[f] = initial[f] + ahead * change

        @pl.when(step < 3)
        def _():
            width_blocks(mirrored(state), send_a, parts_a, send_forward)
            for f in range(fields):
                halo_out[0, pl.ds(f, 1), :] = state[f, pl.ds(0, 1), :]
                halo_out[1, pl.ds(f, 1), :] = state[f, pl.ds(rows - 1, 1), :]
            for copy in halo_copies(step + 1):
                copy.start()

        @pl.when(step == 0)
        def _():
            field_ref[...] = local_field[...]

        return carry

    lax.fori_loop(0, 4, stage, 0)


def local(magnet, window_shift, region, material, kernel):
    components, layers, rows, width = magnet.shape
    grid_y = lax.axis_size("gy")
    devices = lax.axis_size("gx") * grid_y
    fields = components * layers
    track = rows * devices
    freqs = kernel.shape[2]
    groups = 1
    padded = -(-fields // groups * 2 * freqs // lane_tile) * lane_tile
    tables = (*width_tables(width, devices, 2 * track), *track_tables(track))
    vmem = pl.BlockSpec(memory_space=pltpu.VMEM)
    cells = (fields, rows, width)
    half = layers // 2
    blocks = (groups, devices, rows, padded)
    out = pltpu.VMEM((2, *cells), f32)
    dma = pltpu.SemaphoreType.DMA
    both = pl.pallas_call(
        functools.partial(kernel_body, grid_y, devices, layers),
        out_shape=out,
        in_specs=[pl.BlockSpec(memory_space=pltpu.HBM)] * 8 + [pl.BlockSpec(memory_space=pltpu.SMEM)],
        out_specs=vmem,
        scratch_shapes=[
            pltpu.VMEM(cells, f32),
            pltpu.VMEM(tables[0].shape, bf16),
            pltpu.VMEM(kernel.shape, f32),
            *[pltpu.VMEM(table.shape, bf16) for table in tables[1:]],
            pltpu.SMEM(material.shape, f32),
            pltpu.VMEM(region.shape, jnp.int32),
            dma((8,)),
            pltpu.VMEM((fields, 2 * rows, width), f32),
            pltpu.VMEM(cells, f32),
            pltpu.VMEM(cells, f32),
            pltpu.VMEM(cells, f32),
            pltpu.VMEM(cells, f32),
            pltpu.VMEM((2, fields, width), f32),
            pltpu.VMEM((2, 2, fields, width), f32),
            pltpu.VMEM((fields // groups * rows, 2 * width), f32),
            pltpu.VMEM((6, half, half, 2, freqs, 2 * track), f32),
            pltpu.VMEM(blocks, f32),
            pltpu.VMEM(blocks, f32),
            pltpu.VMEM(blocks, f32),
            pltpu.VMEM(blocks, f32),
            pltpu.VMEM((groups * padded, 2 * track), f32),
            pltpu.VMEM((groups * padded, 2 * track), f32),
            pltpu.VMEM((groups, rows, padded), f32),
            dma((2,)),
            dma((2, 2, 2)),
            dma((2,)),
            dma((2,)),
            dma((2,)),
            dma((2,)),
        ],
        compiler_params=pltpu.CompilerParams(
            collective_id=0, has_side_effects=True, vmem_limit_bytes=60 * 2**20
        ),
    )(
        magnet.reshape(cells),
        jnp.asarray(tables[0]),
        kernel,
        *[jnp.asarray(table) for table in tables[1:]],
        material,
        region,
        window_shift,
    )
    return both[0].reshape(magnet.shape), both[1].reshape(magnet.shape)


def solution(mesh):
    cells = P(None, None, ("run", "gx", "gy"), None)
    in_specs = (
        cells,
        P("run"),
        P(("run", "gx", "gy"), None),
        P(),
        P(None, None, ("gx", "gy"), None),
    )
    return jax.shard_map(
        local, mesh=mesh, in_specs=in_specs, out_specs=(cells, cells), check_vma=False
    )
```
